32 devices in a mesh: gx: 4 (over z), gy: 2 (over y), gz: 4 (over x, core).
Axes of the slice: x: 2, y: 2, z: 4, core: 2. Of those that a mesh axis runs over, the one named last changes fastest.
Arguments:
- positions: float32 [3, 8, 4, 32, 128], P(None, 'gx', 'gy', 'gz'), may hold values from 0 to 1
- shield: float32 [8, 4, 32, 128], P('gx', 'gy', 'gz'), may hold values from 0.3 to 1
- width: float32 [8, 4, 32, 128], P('gx', 'gy', 'gz'), may hold values from 0.5 to 2
- hardness: float32 [8, 4, 32, 128], P('gx', 'gy', 'gz'), may hold values from 0.5 to 2
- softness: float32 [8, 4, 32, 128], P('gx', 'gy', 'gz'), may hold values from 0.5 to 2
- coupling: float32 [8, 4, 32, 128], P('gx', 'gy', 'gz'), may hold values from -0.45 to 0.45
- pair_bits: int32 [8, 4, 32], P('gx', 'gy', 'gz'), may hold values from 8192 to 134217727, as said below
- right_side: float32 [4, 8, 4, 32, 128], P(None, 'gx', 'gy', 'gz'), may hold values from -7 to 7
Outputs:
- solution: float32 [4, 8, 4, 32, 128], P(None, 'gx', 'gy', 'gz')
- residual: float32 [4, 8, 4, 32, 128], P(None, 'gx', 'gy', 'gz')
The draws below stay inside these ranges and needn't reach their ends.
Inputs may be any that keep to these rules, and one draw needn't show every extreme that they name: `pair_bits`: bit k of a tile's word stands for the offset with code k as in the reference program; bit 13 is always 1, bits 27 and up are 0, a bit is 0 where the offset leaves the grid, and the lists are symmetric: bit k of tile t equals bit 26 - k of the tile at t plus that offset.
All inputs are finite; a program needn't handle non-finite values.
Results may differ from the reference program's by a relative error of at most 0.0018.
Values sent between devices are 32-bit elements; how exact they have to be, the bound alone decides.
A program may use at most 128 MiB of HBM per device.

```python
import math
import jax
import jax.numpy as jnp
from jax import lax

TILE = 128
ITERS = 3
NTX = 8
NTY = 4
NTZ = 32


def draw_pair_bits(key, part):
    forward_bits = jax.random.randint(key, (NTX, NTY, NTZ, 13), 0, 2).astype(jnp.int32)
    padded_bits = jnp.pad(forward_bits, ((1, 1), (1, 1), (1, 1), (0, 0)))
    index_first = lax.broadcasted_iota(jnp.int32, (NTX, NTY, NTZ), 0)
    index_second = lax.broadcasted_iota(jnp.int32, (NTX, NTY, NTZ), 1)
    index_third = lax.broadcasted_iota(jnp.int32, (NTX, NTY, NTZ), 2)
    packed = jnp.full((NTX, NTY, NTZ), 1 << 13, jnp.int32)
    for offset_code in range(27):
        shift_first = offset_code // 9 - 1
        shift_second = offset_code // 3 % 3 - 1
        shift_third = offset_code % 3 - 1
        if offset_code > 13:
            inside = (index_first + shift_first >= 0) & (index_first + shift_first < NTX)
            inside = inside & (index_second + shift_second >= 0) & (index_second + shift_second < NTY)
            inside = inside & (index_third + shift_third >= 0) & (index_third + shift_third < NTZ)
            chosen = jnp.where(inside, forward_bits[:, :, :, offset_code - 14], 0)
            packed = packed + chosen * (1 << offset_code)
        elif offset_code < 13:
            chosen = padded_bits[1 + shift_first:1 + shift_first + NTX, 1 + shift_second:1 + shift_second + NTY, 1 + shift_third:1 + shift_third + NTZ, 12 - offset_code]
            packed = packed + chosen * (1 << offset_code)
    return packed


def draw_right_side(key, part):
    rough_key = jax.random.fold_in(key, 11)
    sign_key = jax.random.fold_in(key, 12)
    wave_key = jax.random.fold_in(key, 13)
    phase_key = jax.random.fold_in(key, 14)
    shape = (4, NTX, NTY, NTZ, TILE)
    rough = jnp.clip(jax.random.normal(rough_key, shape, jnp.float32), -4.0, 4.0)
    signs = jnp.where(jax.random.bernoulli(sign_key, 0.5, (4,)), 1.0, -1.0).astype(jnp.float32)
    waves = jax.random.randint(wave_key, (4, 3), 1, 3).astype(jnp.float32)
    phases = jax.random.uniform(phase_key, (4,), jnp.float32, -math.pi, math.pi)
    coord_first = (lax.broadcasted_iota(jnp.float32, (NTX, NTY, NTZ), 0) + 0.5) / NTX
    coord_second = (lax.broadcasted_iota(jnp.float32, (NTX, NTY, NTZ), 1) + 0.5) / NTY
    coord_third = (lax.broadcasted_iota(jnp.float32, (NTX, NTY, NTZ), 2) + 0.5) / NTZ
    phase_field = waves[:, 0, None, None, None] * coord_first[None] + waves[:, 1, None, None, None] * coord_second[None] + waves[:, 2, None, None, None] * coord_third[None]
    phase_field = 2.0 * math.pi * phase_field + phases[:, None, None, None]
    smooth = signs[:, None, None, None] * (1.0 + 0.5 * jnp.cos(phase_field))
    return (rough + smooth[..., None]).astype(jnp.float32)


def level_of(own_key, dims, pieces, low, top_value):
    def one(position, parts):
        steps = jax.random.uniform(jax.random.fold_in(jax.random.fold_in(own_key, 6), position), (parts,), jnp.float32, low / len(pieces), top_value / len(pieces))
        return jnp.repeat(jnp.exp(steps), dims[position] // parts).reshape((-1,) + (1,) * (len(dims) - position - 1))

    factor_of = one(*pieces[0])
    for cut in pieces[1:]:
        factor_of = factor_of * one(*cut)
    return factor_of


def setup_inputs(seed: int = 0) -> dict:
    key_of = jax.random.split(jax.random.key(seed), 9)
    positions = jnp.clip(1.0 * jax.random.uniform(key_of[0], (3, NTX, NTY, NTZ, TILE), jnp.float32) ** level_of(key_of[0], (3, NTX, NTY, NTZ, TILE), ((1, 4), (2, 2), (3, 4)), -0.2, 0.2), 0.0, 1.0)
    shield = jnp.clip(jnp.exp(math.log(1.0) - 1.2039728 * jax.random.uniform(key_of[1], (NTX, NTY, NTZ, TILE), jnp.float32) ** level_of(key_of[1], (NTX, NTY, NTZ, TILE), ((0, 4), (1, 2), (2, 4)), -0.2, 0.2)), 0.3, 1.0)
    width = jnp.clip(jnp.exp(math.log(2.0) - 1.3862944 * jax.random.uniform(key_of[2], (NTX, NTY, NTZ, TILE), jnp.float32) ** level_of(key_of[2], (NTX, NTY, NTZ, TILE), ((0, 4), (1, 2), (2, 4)), -0.2, 0.2)), 0.5, 2.0)
    hardness = jnp.clip(jnp.exp(math.log(2.0) - 1.3862944 * jax.random.uniform(key_of[3], (NTX, NTY, NTZ, TILE), jnp.float32) ** level_of(key_of[3], (NTX, NTY, NTZ, TILE), ((0, 4), (1, 2), (2, 4)), -0.2, 0.2)), 0.5, 2.0)
    softness = jnp.clip(jnp.exp(math.log(2.0) - 1.3862944 * jax.random.uniform(key_of[4], (NTX, NTY, NTZ, TILE), jnp.float32) ** level_of(key_of[4], (NTX, NTY, NTZ, TILE), ((0, 4), (1, 2), (2, 4)), -0.2, 0.2)), 0.5, 2.0)
    coupling = jnp.clip(jax.random.uniform(key_of[5], (NTX, NTY, NTZ, TILE), jnp.float32, -0.45, 0.45) * level_of(key_of[5], (NTX, NTY, NTZ, TILE), ((0, 4), (1, 2), (2, 4)), -0.4, 0.0), -0.45, 0.45)
    pair_bits = draw_pair_bits(jax.random.fold_in(key_of[8], 71), 0)
    right_side = draw_right_side(jax.random.fold_in(key_of[8], 71), 0)
    return dict(positions=positions, shield=shield, width=width, hardness=hardness, softness=softness, coupling=coupling, pair_bits=pair_bits, right_side=right_side)


coulomb_scale = 0.002
response_scale = 0.003

def index_tuple(values):
    return tuple((jnp.asarray(value).astype(jnp.int32) for value in values))

def pair_terms(own_params, partner, offset_code, own_bits):
    shift_first = (offset_code // 9 - 1).astype(jnp.float32)
    shift_second = (offset_code // 3 % 3 - 1).astype(jnp.float32)
    shift_third = (offset_code % 3 - 1).astype(jnp.float32)

    def separation(column, shift):
        return shift + (partner[column][:, None, :] - own_params[column][:, :, None])
    first = separation(0, shift_first)
    second = separation(1, shift_second)
    third = separation(2, shift_third)
    distance = first * first + second * second + third * third
    coulomb = coulomb_scale * lax.rsqrt(distance + own_params[3][:, :, None] * partner[3][:, None, :])
    response = response_scale * jnp.exp(-distance / (own_params[4][:, :, None] + partner[4][:, None, :]))
    listed = jnp.right_shift(own_bits, offset_code) & 1 > 0
    tile_size = own_params.shape[2]
    diagonal_mask = lax.broadcasted_iota(jnp.int32, (tile_size, tile_size), 0) == lax.broadcasted_iota(jnp.int32, (tile_size, tile_size), 1)
    kept = listed[:, None, None] & jnp.logical_not(diagonal_mask[None] & (offset_code == 13))
    empty_pair = jnp.zeros_like(distance)
    return (jnp.where(kept, coulomb, empty_pair).astype(jnp.bfloat16), jnp.where(kept, response, empty_pair).astype(jnp.bfloat16))

def inner(vector, other_vector):
    return lax.optimization_barrier(jnp.sum((vector * other_vector).reshape(2, 2, -1), axis=(0, 2)))

def widen(scalars):
    return jnp.concatenate([scalars, scalars]).reshape(4, 1, 1, 1, 1)

def reference(positions, shield, width, hardness, softness, coupling, pair_bits, right_side):
    tiles_x, tiles_y, tiles_z, tile_size = hardness.shape
    params = jnp.concatenate([positions, shield[None], width[None]], axis=0)
    params_pad = jnp.pad(params, ((0, 0), (1, 1), (1, 1), (1, 1), (0, 0)))
    plane = tiles_y * tiles_z

    def operate(vector):
        vector_pad = jnp.pad(vector, ((0, 0), (1, 1), (1, 1), (1, 1), (0, 0)))

        def slab_terms(slab_index):
            slab_index = slab_index.astype(jnp.int32)
            own_params = lax.dynamic_slice(params_pad, index_tuple((0, slab_index + 1, 1, 1, 0)), (5, 1, tiles_y, tiles_z, tile_size)).reshape(5, plane, tile_size)
            own_bits = lax.dynamic_slice(pair_bits, index_tuple((slab_index, 0, 0)), (1, tiles_y, tiles_z)).reshape(plane)

            def visit(offset_code, carry):
                row_coulomb, row_response, pair_charge, pair_potential = carry
                offset_code = offset_code.astype(jnp.int32)
                start = index_tuple((0, slab_index + offset_code // 9, offset_code // 3 % 3, offset_code % 3, 0))
                partner = lax.dynamic_slice(params_pad, start, (5, 1, tiles_y, tiles_z, tile_size)).reshape(5, plane, tile_size)
                neighbour = lax.dynamic_slice(vector_pad, start, (4, 1, tiles_y, tiles_z, tile_size)).reshape(4, plane, tile_size)
                coulomb, response = pair_terms(own_params, partner, offset_code, own_bits)
                coulomb = coulomb.astype(jnp.float32)
                response = response.astype(jnp.float32)
                row_coulomb = row_coulomb + lax.optimization_barrier(jnp.sum(coulomb, axis=2))
                row_response = row_response + lax.optimization_barrier(jnp.sum(response, axis=2))
                pair_charge = pair_charge + jnp.einsum('tij,ftj->fti', coulomb, neighbour[:2], precision=lax.Precision.HIGHEST)
                pair_potential = pair_potential + jnp.einsum('tij,ftj->fti', response, neighbour[2:], precision=lax.Precision.HIGHEST)
                return (row_coulomb, row_response, pair_charge, pair_potential)
            flat_zeros = jnp.zeros((plane, tile_size), jnp.float32)
            pair_zeros = jnp.zeros((2, plane, tile_size), jnp.float32)
            return lax.fori_loop(0, 27, visit, (flat_zeros, flat_zeros, pair_zeros, pair_zeros))
        row_coulomb, row_response, pair_charge, pair_potential = lax.map(slab_terms, jnp.arange(tiles_x, dtype=jnp.int32))
        grid = (tiles_x, tiles_y, tiles_z, tile_size)
        row_coulomb = row_coulomb.reshape(grid)
        row_response = row_response.reshape(grid)
        pair_charge = pair_charge.transpose(1, 0, 2, 3).reshape((2,) + grid)
        pair_potential = pair_potential.transpose(1, 0, 2, 3).reshape((2,) + grid)
        image_charge = (hardness + row_coulomb) * vector[:2] + pair_charge + coupling * vector[2:]
        image_potential = (softness + row_response) * vector[2:] - pair_potential + coupling * vector[:2]
        return jnp.concatenate([image_charge, image_potential], axis=0)
    solution = jnp.zeros_like(right_side)
    remainder = right_side
    direction = right_side
    norm_now = inner(remainder, remainder)
    for iteration in range(ITERS):
        applied = operate(direction)
        step_size = norm_now / inner(direction, applied)
        solution = solution + widen(step_size) * direction
        remainder = remainder - widen(step_size) * applied
        norm_next = inner(remainder, remainder)
        direction = remainder + widen(norm_next / norm_now) * direction
        norm_now = norm_next
    residual = right_side - operate(solution)
    return (solution, residual)
```

```python
import functools
import itertools
import math

import jax
import jax.numpy as jnp
from jax import lax
from jax.experimental import pallas as pl
from jax.experimental.pallas import tpu as pltpu
from jax.sharding import PartitionSpec as P

ITERS = 3
AXES = ("gx", "gy", "gz")
DIRECTIONS = [d for d in itertools.product((-1, 0, 1), repeat=3) if d != (0, 0, 0)]

LOG2E = math.log2(math.e)
coulomb_scale = 0.002 * math.sqrt(LOG2E)
response_scale = 0.003
SHIFT = 2.5


def sides(step, count, unit):
    if step < 0:
        return pl.ds(unit, unit), pl.ds((count + 1) * unit, unit)
    if step > 0:
        return pl.ds(count * unit, unit), pl.ds(0, unit)
    return pl.ds(unit, count * unit), pl.ds(unit, count * unit)


def kernel(
    counts, extent, tile,
    bits_ref, pos_ref, shield_ref, width_ref, hard_ref, soft_ref, coup_ref, rhs_ref,
    sol_ref, res_ref,
    store, par, basis, last, lhs, feats, shields, widths, acc, diag, sums, parts,
    halo_send, halo_recv, sum_send, sum_recv,
):
    tx, ty, tz = extent
    bf16, f32 = jnp.bfloat16, jnp.float32
    me = [lax.axis_index(axis) for axis in AXES]
    inside = pl.ds(tile, tz * tile)

    def lanes(c, n=1):
        if isinstance(c, int):
            return pl.ds(c * tile, n * tile)
        return pl.ds(pl.multiple_of(c * tile, tile), n * tile)

    def exists(d):
        ok = None
        for m, step, count in zip(me, d, counts):
            if step:
                here = (m + step >= 0) & (m + step < count)
                ok = here if ok is None else ok & here
        return ok

    def halo_copy(ref, slot, index, d):
        pairs = [sides(s, n, u) for s, n, u in zip(d, extent, (1, 1, tile))]
        source = (pairs[0][0], pairs[1][0], slice(None), pairs[2][0])
        target = (pairs[0][1], pairs[1][1], slice(None), pairs[2][1])
        return pltpu.make_async_remote_copy(
            src_ref=ref.at[source],
            dst_ref=ref.at[target],
            send_sem=halo_send.at[slot, index],
            recv_sem=halo_recv.at[slot, index],
            device_id=tuple(m + s for m, s in zip(me, d)),
            device_id_type=pl.DeviceIdType.MESH,
        )

    def halo_start(ref, slot):
        for index, d in enumerate(DIRECTIONS):
            @pl.when(exists(d))
            def _():
                halo_copy(ref, slot, index, d).start()

    def halo_fill(ref, fill):
        for d in DIRECTIONS:
            back = tuple(-s for s in d)
            strips = [sides(s, n, u)[1] for s, n, u in zip(back, extent, (1, 1, tile))]

            @pl.when(jnp.logical_not(exists(d)))
            def _():
                region = (strips[0], strips[1], slice(None), strips[2])
                ref[region] = jnp.full(ref.at[region].shape, fill, f32)

    def halo_wait(ref, slot):
        for index, d in enumerate(DIRECTIONS):
            @pl.when(exists(d))
            def _():
                halo_copy(ref, slot, index, d).wait_send()

            back = tuple(-s for s in d)

            @pl.when(exists(back))
            def _():
                halo_copy(ref, slot, index, d).wait_recv()

    rank = (me[0] * counts[1] + me[1]) * counts[2] + me[2]
    hops = [h for h in itertools.product(*map(range, counts)) if any(h)]

    def sum_copies(slot):
        return [
            pltpu.make_async_remote_copy(
                src_ref=sums.at[slot],
                dst_ref=parts.at[slot, rank],
                send_sem=sum_send.at[slot, j],
                recv_sem=sum_recv.at[slot, j],
                device_id=tuple(lax.rem(m + h, n) for m, h, n in zip(me, hop, counts)),
                device_id_type=pl.DeviceIdType.MESH,
            )
            for j, hop in enumerate(hops)
        ]

    column = lax.broadcasted_iota(jnp.int32, (4, tile), 1)

    def sum_start(slot, values):
        packed = jnp.zeros((4, tile), f32)
        for place, value in values.items():
            total = jnp.sum(value, axis=1, keepdims=True)
            packed = jnp.where(column == place, total, packed)
        sums[slot] = packed
        parts[slot, rank] = packed
        for copy in sum_copies(slot):
            copy.start()

    def sum_finish(slot, places):
        for copy in sum_copies(slot):
            copy.wait()
        value = jnp.sum(parts[slot], axis=0)
        value = value + jnp.concatenate([value[2:4], value[0:2]], axis=0)
        return {
            place: jnp.sum(jnp.where(column == place, value, 0.0), axis=1, keepdims=True)
            for place in places
        }

    row = lax.broadcasted_iota(jnp.int32, (8, tile), 0)
    blank = jnp.zeros((3, tile), f32)
    for a, b, c in itertools.product(range(tx), range(ty), range(tz)):
        par[a + 1, b + 1, :, lanes(c + 1)] = jnp.concatenate(
            [
                pos_ref[:, a, b, c, :] - 0.5,
                shield_ref[a, b, c : c + 1, :] * math.sqrt(LOG2E),
                width_ref[a, b, c : c + 1, :],
                blank,
            ],
            axis=0,
        )
        basis[0, a + 1, b + 1, :, lanes(c + 1)] = rhs_ref[:, a, b, c, :]
    halo_start(par, 0)
    halo_start(basis.at[0], 1)
    halo_fill(par, 0.5)
    for k in range(ITERS):
        halo_fill(basis.at[k], 0.0)

    def rounded(value):
        return value.astype(bf16).astype(f32)

    def prepare(ap, bp, cp):
        raw = par[ap, bp, :, lanes(cp)]
        scaled = raw * (2 * LOG2E)
        high = rounded(scaled)
        low = scaled - high
        squares = raw * raw
        norm = (squares[0:1] + squares[1:2] + squares[2:3]) * -LOG2E
        norm_high = rounded(norm)
        first = jnp.where(
            row < 3, high, jnp.where(row == 3, norm_high, jnp.where(row == 4, norm - norm_high, 1.0))
        )
        second = jnp.where(row < 3, high, 0.0)
        third = jnp.where(row < 3, low, 0.0)
        turned = jnp.concatenate([first, second, third, third, raw], axis=0).T
        feats[cp] = turned[:, :32].astype(bf16)
        shields[cp] = jnp.broadcast_to(turned[:, 35:36], (tile, tile))
        widths[cp] = jnp.broadcast_to(turned[:, 36:37], (tile, tile))

    same = lax.broadcasted_iota(jnp.int32, (tile, tile), 0) == lax.broadcasted_iota(
        jnp.int32, (tile, tile), 1
    )

    def pair_rows(ap, bp, a, b, sources):
        oa, ob = ap - 1 - a, bp - 1 - b
        fa, fb = oa.astype(f32), ob.astype(f32)
        offset = jnp.where(row == 0, fa, jnp.where(row == 1, fb, 0.0))
        group = (oa + 1) * 3 + (ob + 1)
        centre = group == 4
        base = (a * ty + b) * tz

        def target(c):
            own = par[a + 1, b + 1, :, lanes(c + 1)]
            grid = jnp.round(own * 128.0) * (1.0 / 128.0)
            rest = own - grid
            moved = own - offset
            squares = moved * moved
            plane = squares[0:1] + squares[1:2]
            bits = bits_ref[a, b, c]
            return own, grid - offset, jnp.where(row < 3, rest, 0.0), plane, own[2:3], bits

        def factors(parts_of, step):
            own, grid, rest, plane, height, bits = parts_of
            shifted = jnp.where(row == 2, grid - float(step), grid)
            norm = (plane + (height - float(step)) * (height - float(step))) * -LOG2E
            norm_high = rounded(norm)
            listed = (jnp.right_shift(bits, group * 3 + (step + 1)) & 1) == 1
            mask = jnp.where(listed, 0.0, -jnp.inf)
            first = jnp.where(row < 3, shifted, jnp.where(row < 5, 1.0, mask))
            first = jnp.where(row == 5, norm_high, jnp.where(row == 6, norm - norm_high, first))
            third = jnp.where(row < 3, shifted, 0.0)
            return jnp.concatenate([first, rest, third, rest], axis=0).astype(bf16)

        held = {}
        for cp in sources:
            cells = [c for c in (cp - 2, cp - 1, cp) if 0 <= c < tz]
            for c in cells:
                if c not in held:
                    held[c] = target(c)
            right = jnp.concatenate([factors(held[c], cp - 1 - c) for c in cells], axis=1)
            got = jnp.dot(feats[cp], right, preferred_element_type=f32)
            for n, c in enumerate(cells):
                own = held[c][0]
                energy = got[:, n * tile : (n + 1) * tile]
                reach = (shields[cp] * own[3:4] - energy).astype(bf16)
                span = (widths[cp] + own[4:5]).astype(bf16)
                coulomb = lax.rsqrt(reach)
                response = jnp.exp2(energy.astype(bf16) / span)
                if cp - 1 == c:
                    drop = same & centre
                    coulomb = jnp.where(drop, jnp.zeros_like(coulomb), coulomb)
                    response = jnp.where(drop, jnp.zeros_like(response), response)
                start = group * (3 * tile) + (cp - c) * tile
                rows = pl.ds(pl.multiple_of(start, tile), tile)
                store[base + c, rows, 0:tile] = coulomb
                store[base + c, rows, tile : 2 * tile] = response

    def source_row(ap, bp, sources):
        for cp in sources:
            prepare(ap, bp, cp)
        a_low, b_low = jnp.maximum(ap - 2, 0), jnp.maximum(bp - 2, 0)
        wide = jnp.minimum(bp, ty - 1) + 1 - b_low
        total = (jnp.minimum(ap, tx - 1) + 1 - a_low) * wide

        def step(n, carry):
            pair_rows(ap, bp, a_low + n // wide, b_low + n % wide, sources)
            return carry

        lax.fori_loop(0, total, step, 0)

    def own_rows(sources):
        def over(q, carry):
            source_row(1 + q // ty, 1 + q % ty, sources)
            return carry

        lax.fori_loop(0, tx * ty, over, 0)

    own_rows(list(range(1, tz + 1)))
    halo_wait(par, 0)
    own_rows([0, tz + 1])

    def ghost_row(q, carry):
        ap = q // (ty + 2)
        bp = q % (ty + 2)
        own = (ap >= 1) & (ap <= tx) & (bp >= 1) & (bp <= ty)
        held = (ap + me[0] >= 1) & (ap + me[0] <= tx + counts[0] - 1)
        held = held & (bp + me[1] >= 1) & (bp + me[1] <= ty + counts[1] - 1)

        @pl.when(jnp.logical_not(own) & held)
        def _():
            source_row(ap, bp, list(range(tz + 2)))

        return carry

    lax.fori_loop(0, (tx + 2) * (ty + 2), ghost_row, 0)

    def split(value):
        upper = rounded(value)
        ones = jnp.ones((8, value.shape[1]), f32)
        return jnp.concatenate([upper, value - upper, ones], axis=0).astype(bf16)

    def split_all(k):
        def one(q, carry):
            ap = q // (ty + 2)
            bp = q % (ty + 2)
            lhs[ap, bp] = split(basis[k, ap, bp])
            return carry

        lax.fori_loop(0, (tx + 2) * (ty + 2), one, 0)

    charge_rows = lax.broadcasted_iota(jnp.int32, (4, tile), 0) < 2
    low_side = [m > 0 for m in me]
    high_side = [m < n - 1 for m, n in zip(me, counts)]

    def near(place, count):
        return [p for p in (place, place + 1, place + 2)], count

    def operate(k):
        norm = product = jnp.zeros((4, tile), f32)
        for a, b in itertools.product(range(tx), range(ty)):
            groups = {}
            for ap, bp in itertools.product(range(a, a + 3), range(b, b + 3)):
                key = (
                    -1 if ap == 0 else int(ap == tx + 1),
                    -1 if bp == 0 else int(bp == ty + 1),
                )
                groups.setdefault(key, []).append((ap, bp))
            base = (a * ty + b) * tz

            def gather(pairs, c, first):
                left = jnp.concatenate([lhs[ap, bp, :, lanes(c, 3)] for ap, bp in pairs], axis=1)
                right = jnp.concatenate(
                    [
                        store[base + c, pl.ds(((ap - a) * 3 + bp - b) * 3 * tile, 3 * tile), :]
                        for ap, bp in pairs
                    ],
                    axis=0,
                )
                got = jnp.dot(left, right, preferred_element_type=f32)
                acc[c] = got if first else acc[c] + got

            for c in range(tz):
                gather(groups[0, 0], c, True)
            for key, pairs in groups.items():
                if key == (0, 0):
                    continue
                there = None
                for m, step in enumerate(key):
                    if step:
                        side = (low_side if step < 0 else high_side)[m]
                        there = side if there is None else there & side

                @pl.when(there)
                def _():
                    for c in range(tz):
                        gather(pairs, c, False)

            for c in range(tz):
                got = acc[c]
                pair = got[0:4] + got[4:8]
                pair = jnp.where(
                    charge_rows, pair[:, :tile] * coulomb_scale, pair[:, tile:] * -response_scale
                )
                here = lanes(c)
                if k == 0:
                    row_sums = jnp.where(
                        charge_rows,
                        got[8:12, :tile] * coulomb_scale + hard_ref[a, b, c : c + 1, :],
                        got[8:12, tile:] * response_scale + soft_ref[a, b, c : c + 1, :],
                    )
                    diag[a, b, :, here] = row_sums - SHIFT
                vector = basis[k, a + 1, b + 1, :, lanes(c + 1)]
                swapped = jnp.concatenate([vector[2:4], vector[0:2]], axis=0)
                link = coup_ref[a, b, c : c + 1, :]
                image = diag[a, b, :, here] * vector + pair + link * swapped
                if k + 1 < ITERS:
                    basis[k + 1, a + 1, b + 1, :, lanes(c + 1)] = image
                else:
                    last[a, b, :, here] = image
                norm = norm + image * image
                product = product + vector * image
        return norm, product

    start_norm = jnp.zeros((4, tile), f32)
    for a, b, c in itertools.product(range(tx), range(ty), range(tz)):
        value = basis[0, a + 1, b + 1, :, lanes(c + 1)]
        start_norm = start_norm + value * value
    moments = {0: start_norm}
    for k in range(ITERS):
        halo_wait(basis.at[k], 1 + k)
        split_all(k)
        norm, product = operate(k)
        moments[2 * k + 1] = product
        if k + 1 < ITERS:
            moments[2 * k + 2] = norm
            halo_start(basis.at[k + 1], 2 + k)
        if k + 2 == ITERS:
            sum_start(0, moments)
            early, moments = list(moments), {}
    sum_start(1, moments)
    gram = sum_finish(0, early)
    gram.update(sum_finish(1, list(moments)))
    gram = {n: jnp.broadcast_to(value, (4, tile)) for n, value in gram.items()}

    def dot(left, right):
        total = None
        for (i, x), (j, y) in itertools.product(enumerate(left), enumerate(right)):
            term = x * y * gram[i + j]
            total = term if total is None else total + term
        return total

    def combined(left, scale, right):
        size = max(len(left), len(right))
        out = []
        for i in range(size):
            if i >= len(left):
                out.append(scale * right[i])
            elif i >= len(right):
                out.append(left[i])
            else:
                out.append(left[i] + scale * right[i])
        return out

    one = jnp.ones((4, tile), f32)
    rem, along, found = [one], [one], []
    norm_now = gram[0]
    for k in range(ITERS):
        image = combined([SHIFT * x for x in along], one, [jnp.zeros_like(one)] + along)
        step_size = norm_now / dot(along, image)
        found = combined(found, step_size, along)
        rem = combined(rem, -step_size, image)
        if k + 1 < ITERS:
            norm_next = dot(rem, rem)
            along = combined(rem, norm_next / norm_now, along)
            norm_now = norm_next

    for a, b, c in itertools.product(range(tx), range(ty), range(tz)):
        held = [basis[k, a + 1, b + 1, :, lanes(c + 1)] for k in range(ITERS)]
        held.append(last[a, b, :, lanes(c)])
        sol_ref[:, a, b, c, :] = sum(x * v for x, v in zip(found, held))
        res_ref[:, a, b, c, :] = sum(x * v for x, v in zip(rem, held))


def on_device(counts, positions, shield, width, hardness, softness, coupling, pair_bits, right_side):
    tx, ty, tz, tile = hardness.shape
    padded = (tx + 2, ty + 2)
    width_lanes = (tz + 2) * tile
    peers = counts[0] * counts[1] * counts[2]
    field = jax.ShapeDtypeStruct((4, tx, ty, tz, tile), jnp.float32)
    vmem = pl.BlockSpec(memory_space=pltpu.VMEM)
    return pl.pallas_call(
        functools.partial(kernel, counts, (tx, ty, tz), tile),
        out_shape=(field, field),
        in_specs=[pl.BlockSpec(memory_space=pltpu.SMEM)] + [vmem] * 7,
        out_specs=(vmem, vmem),
        scratch_shapes=[
            pltpu.VMEM((tx * ty * tz, 27 * tile, 2 * tile), jnp.bfloat16),
            pltpu.VMEM(padded + (8, width_lanes), jnp.float32),
            pltpu.VMEM((ITERS,) + padded + (4, width_lanes), jnp.float32),
            pltpu.VMEM((tx, ty, 4, tz * tile), jnp.float32),
            pltpu.VMEM(padded + (16, width_lanes), jnp.bfloat16),
            pltpu.VMEM((tz + 2, tile, 32), jnp.bfloat16),
            pltpu.VMEM((tz + 2, tile, tile), jnp.float32),
            pltpu.VMEM((tz + 2, tile, tile), jnp.float32),
            pltpu.VMEM((tz, 16, 2 * tile), jnp.float32),
            pltpu.VMEM((tx, ty, 4, tz * tile), jnp.float32),
            pltpu.VMEM((2, 4, tile), jnp.float32),
            pltpu.VMEM((2, peers, 4, tile), jnp.float32),
            pltpu.SemaphoreType.DMA((ITERS + 1, 26)),
            pltpu.SemaphoreType.DMA((ITERS + 1, 26)),
            pltpu.SemaphoreType.DMA((2, peers)),
            pltpu.SemaphoreType.DMA((2, peers)),
        ],
        compiler_params=pltpu.CompilerParams(
            has_side_effects=True, vmem_limit_bytes=67043328
        ),
    )(pair_bits, positions, shield, width, hardness, softness, coupling, right_side)


def solution(mesh):
    counts = tuple(mesh.shape[axis] for axis in AXES)
    tiles = P("gx", "gy", "gz", None)
    four = P(None, "gx", "gy", "gz", None)
    return jax.shard_map(
        functools.partial(on_device, counts),
        mesh=mesh,
        in_specs=(four, tiles, tiles, tiles, tiles, tiles, P("gx", "gy", "gz"), four),
        out_specs=(four, four),
        check_vma=False,
    )
```

```python
import functools
import itertools
import math

import jax
import jax.numpy as jnp
from jax import lax
from jax.experimental import pallas as pl
from jax.experimental.pallas import tpu as pltpu
from jax.sharding import PartitionSpec as P

ITERS = 3
AXES = ("gx", "gy", "gz")
DIRECTIONS = [d for d in itertools.product((-1, 0, 1), repeat=3) if d != (0, 0, 0)]

LOG2E = math.log2(math.e)
coulomb_scale = 0.002 * math.sqrt(LOG2E)
response_scale = 0.003
SHIFT = 2.5


def sides(step, count, unit):
    if step < 0:
        return pl.ds(unit, unit), pl.ds((count + 1) * unit, unit)
    if step > 0:
        return pl.ds(count * unit, unit), pl.ds(0, unit)
    return pl.ds(unit, count * unit), pl.ds(unit, count * unit)


def kernel(
    counts, extent, tile,
    bits_ref, pos_ref, shield_ref, width_ref, hard_ref, soft_ref, coup_ref, rhs_ref,
    sol_ref, res_ref,
    store, par, basis, last, lhs, feats, shields, widths, acc, diag, sums, parts,
    halo_send, halo_recv, sum_send, sum_recv,
):
    tx, ty, tz = extent
    bf16, f32 = jnp.bfloat16, jnp.float32
    me = [lax.axis_index(axis) for axis in AXES]
    inside = pl.ds(tile, tz * tile)

    def lanes(c, n=1):
        if isinstance(c, int):
            return pl.ds(c * tile, n * tile)
        return pl.ds(pl.multiple_of(c * tile, tile), n * tile)

    def exists(d):
        ok = None
        for m, step, count in zip(me, d, counts):
            if step:
                here = (m + step >= 0) & (m + step < count)
                ok = here if ok is None else ok & here
        return ok

    def halo_copy(ref, slot, index, d):
        pairs = [sides(s, n, u) for s, n, u in zip(d, extent, (1, 1, tile))]
        source = (pairs[0][0], pairs[1][0], slice(None), pairs[2][0])
        target = (pairs[0][1], pairs[1][1], slice(None), pairs[2][1])
        return pltpu.make_async_remote_copy(
            src_ref=ref.at[source],
            dst_ref=ref.at[target],
            send_sem=halo_send.at[slot, index],
            recv_sem=halo_recv.at[slot, index],
            device_id=tuple(m + s for m, s in zip(me, d)),
            device_id_type=pl.DeviceIdType.MESH,
        )

    def halo_start(ref, slot):
        for index, d in enumerate(DIRECTIONS):
            @pl.when(exists(d))
            def _():
                halo_copy(ref, slot, index, d).start()

    def halo_fill(ref, fill):
        for d in DIRECTIONS:
            back = tuple(-s for s in d)
            strips = [sides(s, n, u)[1] for s, n, u in zip(back, extent, (1, 1, tile))]

            @pl.when(jnp.logical_not(exists(d)))
            def _():
                region = (strips[0], strips[1], slice(None), strips[2])
                ref[region] = jnp.full(ref.at[region].shape, fill, f32)

    def halo_wait(ref, slot):
        for index, d in enumerate(DIRECTIONS):
            @pl.when(exists(d))
            def _():
                halo_copy(ref, slot, index, d).wait_send()

            back = tuple(-s for s in d)

            @pl.when(exists(back))
            def _():
                halo_copy(ref, slot, index, d).wait_recv()

    rank = (me[0] * counts[1] + me[1]) * counts[2] + me[2]
    hops = [h for h in itertools.product(*map(range, counts)) if any(h)]

    def sum_copies(slot):
        return [
            pltpu.make_async_remote_copy(
                src_ref=sums.at[slot],
                dst_ref=parts.at[slot, rank],
                send_sem=sum_send.at[slot, j],
                recv_sem=sum_recv.at[slot, j],
                device_id=tuple(lax.rem(m + h, n) for m, h, n in zip(me, hop, counts)),
                device_id_type=pl.DeviceIdType.MESH,
            )
            for j, hop in enumerate(hops)
        ]

    column = lax.broadcasted_iota(jnp.int32, (4, tile), 1)

    def sum_start(slot, values):
        packed = jnp.zeros((4, tile), f32)
        for place, value in values.items():
            total = jnp.sum(value, axis=1, keepdims=True)
            packed = jnp.where(column == place, total, packed)
        sums[slot] = packed
        parts[slot, rank] = packed
        for copy in sum_copies(slot):
            copy.start()

    def sum_finish(slot, places):
        for copy in sum_copies(slot):
            copy.wait()
        value = jnp.sum(parts[slot], axis=0)
        value = value + jnp.concatenate([value[2:4], value[0:2]], axis=0)
        return {
            place: jnp.sum(jnp.where(column == place, value, 0.0), axis=1, keepdims=True)
            for place in places
        }

    barrier = pltpu.get_barrier_semaphore()
    for hop in hops:
        pl.semaphore_signal(
            barrier,
            inc=1,
            device_id=tuple(lax.rem(m + h, n) for m, h, n in zip(me, hop, counts)),
            device_id_type=pl.DeviceIdType.MESH,
        )

    row = lax.broadcasted_iota(jnp.int32, (8, tile), 0)
    blank = jnp.zeros((3, tile), f32)
    for a, b, c in itertools.product(range(tx), range(ty), range(tz)):
        par[a + 1, b + 1, :, lanes(c + 1)] = jnp.concatenate(
            [
                pos_ref[:, a, b, c, :] - 0.5,
                shield_ref[a, b, c : c + 1, :] * math.sqrt(LOG2E),
                width_ref[a, b, c : c + 1, :],
                blank,
            ],
            axis=0,
        )
        basis[0, a + 1, b + 1, :, lanes(c + 1)] = rhs_ref[:, a, b, c, :]
    halo_fill(par, 0.5)
    for k in range(ITERS):
        halo_fill(basis.at[k], 0.0)

    def rounded(value):
        return value.astype(bf16).astype(f32)

    def prepare(ap, bp, cp):
        raw = par[ap, bp, :, lanes(cp)]
        scaled = raw * (2 * LOG2E)
        high = rounded(scaled)
        low = scaled - high
        squares = raw * raw
        norm = (squares[0:1] + squares[1:2] + squares[2:3]) * -LOG2E
        norm_high = rounded(norm)
        first = jnp.where(
            row < 3, high, jnp.where(row == 3, norm_high, jnp.where(row == 4, norm - norm_high, 1.0))
        )
        second = jnp.where(row < 3, high, 0.0)
        third = jnp.where(row < 3, low, 0.0)
        turned = jnp.concatenate([first, second, third, third, raw], axis=0).T
        feats[cp] = turned[:, :32].astype(bf16)
        shields[cp] = jnp.broadcast_to(turned[:, 35:36], (tile, tile))
        widths[cp] = jnp.broadcast_to(turned[:, 36:37], (tile, tile))

    same = lax.broadcasted_iota(jnp.int32, (tile, tile), 0) == lax.broadcasted_iota(
        jnp.int32, (tile, tile), 1
    )

    def pair_rows(ap, bp, a, b, sources):
        oa, ob = ap - 1 - a, bp - 1 - b
        fa, fb = oa.astype(f32), ob.astype(f32)
        offset = jnp.where(row == 0, fa, jnp.where(row == 1, fb, 0.0))
        group = (oa + 1) * 3 + (ob + 1)
        centre = group == 4
        base = (a * ty + b) * tz

        def target(c):
            own = par[a + 1, b + 1, :, lanes(c + 1)]
            grid = jnp.round(own * 128.0) * (1.0 / 128.0)
            rest = own - grid
            moved = own - offset
            squares = moved * moved
            plane = squares[0:1] + squares[1:2]
            bits = bits_ref[a, b, c]
            return own, grid - offset, jnp.where(row < 3, rest, 0.0), plane, own[2:3], bits

        def factors(parts_of, step):
            own, grid, rest, plane, height, bits = parts_of
            shifted = jnp.where(row == 2, grid - float(step), grid)
            norm = (plane + (height - float(step)) * (height - float(step))) * -LOG2E
            norm_high = rounded(norm)
            listed = (jnp.right_shift(bits, group * 3 + (step + 1)) & 1) == 1
            mask = jnp.where(listed, 0.0, -jnp.inf)
            first = jnp.where(row < 3, shifted, jnp.where(row < 5, 1.0, mask))
            first = jnp.where(row == 5, norm_high, jnp.where(row == 6, norm - norm_high, first))
            third = jnp.where(row < 3, shifted, 0.0)
            return jnp.concatenate([first, rest, third, rest], axis=0).astype(bf16)

        held = {}
        for cp in sources:
            cells = [c for c in (cp - 2, cp - 1, cp) if 0 <= c < tz]
            for c in cells:
                if c not in held:
                    held[c] = target(c)
            right = jnp.concatenate([factors(held[c], cp - 1 - c) for c in cells], axis=1)
            got = jnp.dot(feats[cp], right, preferred_element_type=f32)
            for n, c in enumerate(cells):
                own = held[c][0]
                energy = got[:, n * tile : (n + 1) * tile]
                reach = (shields[cp] * own[3:4] - energy).astype(bf16)
                span = (widths[cp] + own[4:5]).astype(bf16)
                coulomb = lax.rsqrt(reach)
                response = jnp.exp2(energy.astype(bf16) / span)
                if cp - 1 == c:
                    drop = same & centre
                    coulomb = jnp.where(drop, jnp.zeros_like(coulomb), coulomb)
                    response = jnp.where(drop, jnp.zeros_like(response), response)
                start = group * (3 * tile) + (cp - c) * tile
                rows = pl.ds(pl.multiple_of(start, tile), tile)
                store[base + c, 0, rows, :] = coulomb
                store[base + c, 1, rows, :] = response

    def source_row(ap, bp, sources):
        for cp in sources:
            prepare(ap, bp, cp)
        a_low, b_low = jnp.maximum(ap - 2, 0), jnp.maximum(bp - 2, 0)
        wide = jnp.minimum(bp, ty - 1) + 1 - b_low
        total = (jnp.minimum(ap, tx - 1) + 1 - a_low) * wide

        def step(n, carry):
            pair_rows(ap, bp, a_low + n // wide, b_low + n % wide, sources)
            return carry

        lax.fori_loop(0, total, step, 0)

    def own_rows(first, stop, sources):
        def over(q, carry):
            source_row(1 + q // ty, 1 + q % ty, sources)
            return carry

        lax.fori_loop(first, stop, over, 0)

    own_rows(0, 1, list(range(1, tz + 1)))
    pl.semaphore_wait(barrier, len(hops))
    halo_start(par, 0)
    halo_start(basis.at[0], 1)
    own_rows(1, tx * ty, list(range(1, tz + 1)))
    halo_wait(par, 0)
    own_rows(0, tx * ty, [0, tz + 1])

    def ghost_row(q, carry):
        ap = q // (ty + 2)
        bp = q % (ty + 2)
        own = (ap >= 1) & (ap <= tx) & (bp >= 1) & (bp <= ty)
        held = (ap + me[0] >= 1) & (ap + me[0] <= tx + counts[0] - 1)
        held = held & (bp + me[1] >= 1) & (bp + me[1] <= ty + counts[1] - 1)

        @pl.when(jnp.logical_not(own) & held)
        def _():
            source_row(ap, bp, list(range(tz + 2)))

        return carry

    lax.fori_loop(0, (tx + 2) * (ty + 2), ghost_row, 0)

    def split(value):
        upper = rounded(value)
        ones = jnp.ones((8, value.shape[1]), f32)
        return jnp.concatenate([upper, value - upper, ones], axis=0).astype(bf16)

    def split_rows(k, places, cells):
        for ap, bp in places:
            for cp in cells:
                lhs[k % 2, ap, bp, cp] = split(basis[k, ap, bp, :, lanes(cp)])

    every = list(itertools.product(range(tx + 2), range(ty + 2)))
    own_places = [(ap, bp) for ap, bp in every if 1 <= ap <= tx and 1 <= bp <= ty]
    ghost_places = [p for p in every if p not in own_places]

    def split_ghosts(k):
        split_rows(k, own_places, (0, tz + 1))
        split_rows(k, ghost_places, range(tz + 2))

    charge_rows = lax.broadcasted_iota(jnp.int32, (4, tile), 0) < 2
    low_side = [m > 0 for m in me]
    high_side = [m < n - 1 for m, n in zip(me, counts)]

    def neighbours(a, b):
        groups = {}
        for ap, bp in itertools.product(range(a, a + 3), range(b, b + 3)):
            key = (
                -1 if ap == 0 else int(ap == tx + 1),
                -1 if bp == 0 else int(bp == ty + 1),
            )
            groups.setdefault(key, []).append((ap, bp))
        return groups

    tiles_of = [(a, b, (a * ty + b) * tz) for a, b in itertools.product(range(tx), range(ty))]

    def gather(k, a, b, base, pairs, c, first):
        left = jnp.concatenate(
            [lhs[k % 2, ap, bp, c + n] for ap, bp in pairs for n in range(3)], axis=1
        )
        right = jnp.concatenate(
            [
                jnp.concatenate(
                    [
                        store[base + c, f, pl.ds(((ap - a) * 3 + bp - b) * 3 * tile, 3 * tile), :]
                        for f in range(2)
                    ],
                    axis=1,
                )
                for ap, bp in pairs
            ],
            axis=0,
        )
        got = jnp.dot(left, right, preferred_element_type=f32)
        acc[base + c] = got if first else acc[base + c] + got

    def operate_inside(k):
        for a, b, base in tiles_of:
            for c in range(1, tz - 1):
                gather(k, a, b, base, neighbours(a, b)[0, 0], c, True)

    def operate_outside(k):
        norm = product = jnp.zeros((4, tile), f32)
        for a, b, base in tiles_of:
            groups = neighbours(a, b)
            for c in sorted({0, tz - 1}):
                gather(k, a, b, base, groups[0, 0], c, True)
            for key, pairs in groups.items():
                if key == (0, 0):
                    continue
                there = None
                for m, step in enumerate(key):
                    if step:
                        side = (low_side if step < 0 else high_side)[m]
                        there = side if there is None else there & side

                @pl.when(there)
                def _():
                    for c in range(tz):
                        gather(k, a, b, base, pairs, c, False)

            for c in range(tz):
                got = acc[base + c]
                pair = got[0:4] + got[4:8]
                pair = jnp.where(
                    charge_rows, pair[:, :tile] * coulomb_scale, pair[:, tile:] * -response_scale
                )
                here = lanes(c)
                if k == 0:
                    row_sums = jnp.where(
                        charge_rows,
                        got[8:12, :tile] * coulomb_scale + hard_ref[a, b, c : c + 1, :],
                        got[8:12, tile:] * response_scale + soft_ref[a, b, c : c + 1, :],
                    )
                    diag[a, b, :, here] = row_sums - SHIFT
                vector = basis[k, a + 1, b + 1, :, lanes(c + 1)]
                swapped = jnp.concatenate([vector[2:4], vector[0:2]], axis=0)
                link = coup_ref[a, b, c : c + 1, :]
                image = diag[a, b, :, here] * vector + pair + link * swapped
                if k + 1 < ITERS:
                    basis[k + 1, a + 1, b + 1, :, lanes(c + 1)] = image
                    lhs[(k + 1) % 2, a + 1, b + 1, c + 1] = split(image)
                else:
                    last[a, b, :, here] = image
                norm = norm + image * image
                product = product + vector * image
        return norm, product

    start_norm = jnp.zeros((4, tile), f32)
    for a, b, c in itertools.product(range(tx), range(ty), range(tz)):
        value = basis[0, a + 1, b + 1, :, lanes(c + 1)]
        start_norm = start_norm + value * value
    moments = {0: start_norm}
    split_rows(0, own_places, range(1, tz + 1))
    for k in range(ITERS):
        operate_inside(k)
        halo_wait(basis.at[k], 1 + k)
        split_ghosts(k)
        norm, product = operate_outside(k)
        moments[2 * k + 1] = product
        if k + 1 < ITERS:
            moments[2 * k + 2] = norm
            halo_start(basis.at[k + 1], 2 + k)
        if k + 2 == ITERS:
            sum_start(0, moments)
            early, moments = list(moments), {}
    sum_start(1, moments)
    gram = sum_finish(0, early)
    gram.update(sum_finish(1, list(moments)))
    gram = {n: jnp.broadcast_to(value, (4, tile)) for n, value in gram.items()}

    def dot(left, right):
        total = None
        for (i, x), (j, y) in itertools.product(enumerate(left), enumerate(right)):
            term = x * y * gram[i + j]
            total = term if total is None else total + term
        return total

    def combined(left, scale, right):
        size = max(len(left), len(right))
        out = []
        for i in range(size):
            if i >= len(left):
                out.append(scale * right[i])
            elif i >= len(right):
                out.append(left[i])
            else:
                out.append(left[i] + scale * right[i])
        return out

    one = jnp.ones((4, tile), f32)
    rem, along, found = [one], [one], []
    norm_now = gram[0]
    for k in range(ITERS):
        image = combined([SHIFT * x for x in along], one, [jnp.zeros_like(one)] + along)
        step_size = norm_now / dot(along, image)
        found = combined(found, step_size, along)
        rem = combined(rem, -step_size, image)
        if k + 1 < ITERS:
            norm_next = dot(rem, rem)
            along = combined(rem, norm_next / norm_now, along)
            norm_now = norm_next

    for a, b, c in itertools.product(range(tx), range(ty), range(tz)):
        held = [basis[k, a + 1, b + 1, :, lanes(c + 1)] for k in range(ITERS)]
        held.append(last[a, b, :, lanes(c)])
        sol_ref[:, a, b, c, :] = sum(x * v for x, v in zip(found, held))
        res_ref[:, a, b, c, :] = sum(x * v for x, v in zip(rem, held))


def on_device(counts, positions, shield, width, hardness, softness, coupling, pair_bits, right_side):
    tx, ty, tz, tile = hardness.shape
    padded = (tx + 2, ty + 2)
    width_lanes = (tz + 2) * tile
    peers = counts[0] * counts[1] * counts[2]
    field = jax.ShapeDtypeStruct((4, tx, ty, tz, tile), jnp.float32)
    vmem = pl.BlockSpec(memory_space=pltpu.VMEM)
    return pl.pallas_call(
        functools.partial(kernel, counts, (tx, ty, tz), tile),
        out_shape=(field, field),
        in_specs=[pl.BlockSpec(memory_space=pltpu.SMEM)] + [vmem] * 7,
        out_specs=(vmem, vmem),
        scratch_shapes=[
            pltpu.VMEM((tx * ty * tz, 2, 27 * tile, tile), jnp.bfloat16),
            pltpu.VMEM(padded + (8, width_lanes), jnp.float32),
            pltpu.VMEM((ITERS,) + padded + (4, width_lanes), jnp.float32),
            pltpu.VMEM((tx, ty, 4, tz * tile), jnp.float32),
            pltpu.VMEM((2,) + padded + (tz + 2, 16, tile), jnp.bfloat16),
            pltpu.VMEM((tz + 2, tile, 32), jnp.bfloat16),
            pltpu.VMEM((tz + 2, tile, tile), jnp.float32),
            pltpu.VMEM((tz + 2, tile, tile), jnp.float32),
            pltpu.VMEM((tx * ty * tz, 16, 2 * tile), jnp.float32),
            pltpu.VMEM((tx, ty, 4, tz * tile), jnp.float32),
            pltpu.VMEM((2, 4, tile), jnp.float32),
            pltpu.VMEM((2, peers, 4, tile), jnp.float32),
            pltpu.SemaphoreType.DMA((ITERS + 1, 26)),
            pltpu.SemaphoreType.DMA((ITERS + 1, 26)),
            pltpu.SemaphoreType.DMA((2, peers)),
            pltpu.SemaphoreType.DMA((2, peers)),
        ],
        compiler_params=pltpu.CompilerParams(
            collective_id=0, has_side_effects=True, vmem_limit_bytes=67043328
        ),
    )(pair_bits, positions, shield, width, hardness, softness, coupling, right_side)


def solution(mesh):
    counts = tuple(mesh.shape[axis] for axis in AXES)
    tiles = P("gx", "gy", "gz", None)
    four = P(None, "gx", "gy", "gz", None)
    return jax.shard_map(
        functools.partial(on_device, counts),
        mesh=mesh,
        in_specs=(four, tiles, tiles, tiles, tiles, tiles, P("gx", "gy", "gz"), four),
        out_specs=(four, four),
        check_vma=False,
    )
```

```python
import functools
import itertools
import math

import jax
import jax.numpy as jnp
from jax import lax
from jax.experimental import pallas as pl
from jax.experimental.pallas import tpu as pltpu
from jax.sharding import PartitionSpec as P

ITERS = 3
AXES = ("gx", "gy", "gz")
DIRECTIONS = [d for d in itertools.product((-1, 0, 1), repeat=3) if d != (0, 0, 0)]

LOG2E = math.log2(math.e)
coulomb_scale = 0.002 * math.sqrt(LOG2E)
response_scale = 0.003
SHIFT = 2.5


def sides(step, count, unit):
    if step < 0:
        return pl.ds(unit, unit), pl.ds((count + 1) * unit, unit)
    if step > 0:
        return pl.ds(count * unit, unit), pl.ds(0, unit)
    return pl.ds(unit, count * unit), pl.ds(unit, count * unit)


def kernel(
    counts, extent, tile,
    bits_ref, pos_ref, shield_ref, width_ref, hard_ref, soft_ref, coup_ref, rhs_ref,
    out_ref,
    store, par, basis, last, lhs, feats, columns, picker, energies, acc, diag, sums, parts,
    halo_send, halo_recv, sum_send, sum_recv,
):
    tx, ty, tz = extent
    bf16, f32 = jnp.bfloat16, jnp.float32
    me = [lax.axis_index(axis) for axis in AXES]
    inside = pl.ds(tile, tz * tile)

    def lanes(c, n=1):
        if isinstance(c, int):
            return pl.ds(c * tile, n * tile)
        return pl.ds(pl.multiple_of(c * tile, tile), n * tile)

    def exists(d):
        ok = None
        for m, step, count in zip(me, d, counts):
            if step:
                here = (m + step >= 0) & (m + step < count)
                ok = here if ok is None else ok & here
        return ok

    def halo_copy(ref, slot, index, d):
        pairs = [sides(s, n, u) for s, n, u in zip(d, extent, (1, 1, tile))]
        source = (pairs[0][0], pairs[1][0], slice(None), pairs[2][0])
        target = (pairs[0][1], pairs[1][1], slice(None), pairs[2][1])
        return pltpu.make_async_remote_copy(
            src_ref=ref.at[source],
            dst_ref=ref.at[target],
            send_sem=halo_send.at[slot, index],
            recv_sem=halo_recv.at[slot, index],
            device_id=tuple(m + s for m, s in zip(me, d)),
            device_id_type=pl.DeviceIdType.MESH,
        )

    def halo_start(ref, slot):
        for index, d in enumerate(DIRECTIONS):
            @pl.when(exists(d))
            def _():
                halo_copy(ref, slot, index, d).start()

    def halo_fill(ref, fill):
        for d in DIRECTIONS:
            back = tuple(-s for s in d)
            strips = [sides(s, n, u)[1] for s, n, u in zip(back, extent, (1, 1, tile))]

            @pl.when(jnp.logical_not(exists(d)))
            def _():
                region = (strips[0], strips[1], slice(None), strips[2])
                ref[region] = jnp.full(ref.at[region].shape, fill, f32)

    def halo_wait(ref, slot):
        for index, d in enumerate(DIRECTIONS):
            @pl.when(exists(d))
            def _():
                halo_copy(ref, slot, index, d).wait_send()

            back = tuple(-s for s in d)

            @pl.when(exists(back))
            def _():
                halo_copy(ref, slot, index, d).wait_recv()

    rank = (me[0] * counts[1] + me[1]) * counts[2] + me[2]
    hops = [h for h in itertools.product(*map(range, counts)) if any(h)]

    def sum_copies(slot):
        return [
            pltpu.make_async_remote_copy(
                src_ref=sums.at[slot],
                dst_ref=parts.at[slot, rank],
                send_sem=sum_send.at[slot, j],
                recv_sem=sum_recv.at[slot, j],
                device_id=tuple(lax.rem(m + h, n) for m, h, n in zip(me, hop, counts)),
                device_id_type=pl.DeviceIdType.MESH,
            )
            for j, hop in enumerate(hops)
        ]

    column = lax.broadcasted_iota(jnp.int32, (4, tile), 1)
    field = lax.broadcasted_iota(jnp.int32, (4, tile), 0)

    def sum_start(slot, values):
        packed = jnp.zeros((4, tile), f32)
        for place, value in values.items():
            total = jnp.sum(value, axis=1, keepdims=True)
            packed = jnp.where(column == 4 * place + field, total, packed)
        packed = jnp.sum(packed, axis=0, keepdims=True)
        sums[slot] = packed
        parts[slot, rank] = packed
        for copy in sum_copies(slot):
            copy.start()

    def sum_finish(slot, places):
        for copy in sum_copies(slot):
            copy.wait()
        value = jnp.broadcast_to(jnp.sum(parts[slot], axis=0), (4, tile))
        value = jnp.where(column % 2 == field % 2, value, 0.0)
        return {
            place: jnp.sum(jnp.where(column // 4 == place, value, 0.0), axis=1, keepdims=True)
            for place in places
        }

    barrier = pltpu.get_barrier_semaphore()
    for hop in hops:
        pl.semaphore_signal(
            barrier,
            inc=1,
            device_id=tuple(lax.rem(m + h, n) for m, h, n in zip(me, hop, counts)),
            device_id_type=pl.DeviceIdType.MESH,
        )

    row = lax.broadcasted_iota(jnp.int32, (8, tile), 0)
    blank = jnp.zeros((3, tile), f32)
    for a, b, c in itertools.product(range(tx), range(ty), range(tz)):
        par[a + 1, b + 1, :, lanes(c + 1)] = jnp.concatenate(
            [
                pos_ref[:, a, b, c, :] - 0.5,
                shield_ref[a, b, c : c + 1, :] * math.sqrt(LOG2E),
                width_ref[a, b, c : c + 1, :],
                blank,
            ],
            axis=0,
        )
        basis[0, a + 1, b + 1, :, lanes(c + 1)] = rhs_ref[:, a, b, c, :]
    halo_fill(par, 0.5)
    for k in range(ITERS):
        halo_fill(basis.at[k], 0.0)

    def rounded(value):
        return value.astype(bf16).astype(f32)

    slab = lax.broadcasted_iota(jnp.int32, (32, 2 * tile), 0)
    half = lax.broadcasted_iota(jnp.int32, (32, 2 * tile), 1) // tile
    picker[...] = jnp.where((slab >= 8) & (slab % 8 == 3 + half), 1.0, 0.0).astype(bf16)

    def prepare(ap, bp, cp):
        raw = par[ap, bp, :, lanes(cp)]
        scaled = raw * (2 * LOG2E)
        high = rounded(scaled)
        low = scaled - high
        squares = raw * raw
        norm = (squares[0:1] + squares[1:2] + squares[2:3]) * -LOG2E
        norm_high = rounded(norm)
        first = jnp.where(
            row < 3, high, jnp.where(row == 3, norm_high, jnp.where(row == 4, norm - norm_high, 1.0))
        )
        part = rounded(raw)
        rest = raw - part
        middle = rounded(rest)
        second = jnp.where(row < 3, high, jnp.where(row < 5, part, 0.0))
        third = jnp.where(row < 3, low, jnp.where(row < 5, middle, 0.0))
        fourth = jnp.where(row < 3, low, jnp.where(row < 5, rest - middle, 0.0))
        turned = jnp.concatenate([first, second, third, fourth], axis=0).T.astype(bf16)
        feats[cp] = turned
        columns[cp] = jnp.dot(turned, picker[...], preferred_element_type=f32)

    same = lax.broadcasted_iota(jnp.int32, (tile, tile), 0) == lax.broadcasted_iota(
        jnp.int32, (tile, tile), 1
    )

    def place_of(ap, bp, a, b):
        oa, ob = ap - 1 - a, bp - 1 - b
        group = (oa + 1) * 3 + (ob + 1)
        return oa, ob, group, (a * ty + b) * tz

    def cells_of(cp):
        return [c for c in (cp - 2, cp - 1, cp) if 0 <= c < tz]

    def measure_rows(ap, bp, a, b, sources, slot):
        oa, ob, group, _ = place_of(ap, bp, a, b)
        fa, fb = oa.astype(f32), ob.astype(f32)
        offset = jnp.where(row == 0, fa, jnp.where(row == 1, fb, 0.0))

        def target(c):
            own = par[a + 1, b + 1, :, lanes(c + 1)]
            grid = jnp.round(own * 128.0) * (1.0 / 128.0)
            rest = own - grid
            moved = own - offset
            squares = moved * moved
            plane = squares[0:1] + squares[1:2]
            bits = bits_ref[a, b, c]
            return own, grid - offset, jnp.where(row < 3, rest, 0.0), plane, own[2:3], bits

        def factors(parts_of, step):
            own, grid, rest, plane, height, bits = parts_of
            shifted = jnp.where(row == 2, grid - float(step), grid)
            norm = (plane + (height - float(step)) * (height - float(step))) * -LOG2E
            norm_high = rounded(norm)
            listed = (jnp.right_shift(bits, group * 3 + (step + 1)) & 1) == 1
            mask = jnp.where(listed, 0.0, -jnp.inf)
            first = jnp.where(row < 3, shifted, jnp.where(row < 5, 1.0, mask))
            first = jnp.where(row == 5, norm_high, jnp.where(row == 6, norm - norm_high, first))
            third = jnp.where(row < 3, shifted, 0.0)
            return jnp.concatenate([first, rest, third, rest], axis=0).astype(bf16)

        held = {}
        for cp in sources:
            cells = cells_of(cp)
            for c in cells:
                if c not in held:
                    held[c] = target(c)
            right = jnp.concatenate([factors(held[c], cp - 1 - c) for c in cells], axis=1)
            got = jnp.dot(feats[cp], right, preferred_element_type=f32)
            for m in range(len(cells)):
                energies[slot + m] = got[:, m * tile : (m + 1) * tile]
            slot += len(cells)

    def fill_rows(ap, bp, a, b, sources, slot):
        _, _, group, base = place_of(ap, bp, a, b)
        centre = group == 4
        for cp in sources:
            for c in cells_of(cp):
                own = par[a + 1, b + 1, :, lanes(c + 1)]
                energy = energies[slot].astype(bf16)
                slot += 1
                reach = (columns[cp, :, :tile] * own[3:4]).astype(bf16) - energy
                span = (columns[cp, :, tile:] + own[4:5]).astype(bf16)
                coulomb = lax.rsqrt(reach)
                response = jnp.exp2(energy / span)
                if cp - 1 == c:
                    drop = same & centre
                    coulomb = jnp.where(drop, jnp.zeros_like(coulomb), coulomb)
                    response = jnp.where(drop, jnp.zeros_like(response), response)
                start = group * (3 * tile) + (cp - c) * tile
                rows = pl.ds(pl.multiple_of(start, tile), tile)
                store[base + c, rows, :] = jnp.concatenate([coulomb, response], axis=1)

    def several(ap, bp, places, sources):
        each = sum(len(cells_of(cp)) for cp in sources)
        for n, (a, b) in enumerate(places):
            measure_rows(ap, bp, a, b, sources, n * each)
        for n, (a, b) in enumerate(places):
            fill_rows(ap, bp, a, b, sources, n * each)

    def source_row(ap, bp, sources, least=1):
        for cp in sources:
            prepare(ap, bp, cp)
        a_low, b_low = jnp.maximum(ap - 2, 0), jnp.maximum(bp - 2, 0)
        wide = jnp.minimum(bp, ty - 1) + 1 - b_low
        total = (jnp.minimum(ap, tx - 1) + 1 - a_low) * wide

        def place(n):
            return a_low + n // wide, b_low + n % wide

        def step(n, carry):
            several(ap, bp, [place(least * n + m) for m in range(least)], sources)
            return carry

        def single(n, carry):
            several(ap, bp, [place(total - 1)], sources)
            return carry

        lax.fori_loop(0, total // least, step, 0)
        if least == 2 and not (tx <= 2 and ty <= 2 and len(sources) == tz):
            lax.fori_loop(0, total % 2, single, 0)

    def own_rows(first, stop, sources, least):
        def over(q, carry):
            source_row(1 + q // ty, 1 + q % ty, sources, least)
            return carry

        lax.fori_loop(first, stop, over, 0)

    pairs = 2 if tx == 2 and ty == 2 else 1
    own_rows(0, 1, list(range(1, tz + 1)), pairs)
    pl.semaphore_wait(barrier, len(hops))
    halo_start(par, 0)
    halo_start(basis.at[0], 1)
    own_rows(1, tx * ty, list(range(1, tz + 1)), pairs)
    halo_wait(par, 0)
    own_rows(0, tx * ty, [0, tz + 1], 2 * pairs if pairs == 2 else 1)

    def ghost_row(q, carry):
        ap = q // (ty + 2)
        bp = q % (ty + 2)
        own = (ap >= 1) & (ap <= tx) & (bp >= 1) & (bp <= ty)
        held = (ap + me[0] >= 1) & (ap + me[0] <= tx + counts[0] - 1)
        held = held & (bp + me[1] >= 1) & (bp + me[1] <= ty + counts[1] - 1)

        @pl.when(jnp.logical_not(own) & held)
        def _():
            source_row(ap, bp, list(range(tz + 2)), 2)

        return carry

    lax.fori_loop(0, (tx + 2) * (ty + 2), ghost_row, 0)

    def split(value):
        upper = rounded(value)
        ones = jnp.ones((8, value.shape[1]), f32)
        return jnp.concatenate([upper, value - upper, ones], axis=0).astype(bf16)

    def split_rows(k, places, cells):
        for ap, bp in places:
            for cp in cells:
                lhs[k % 2, ap, bp, cp] = split(basis[k, ap, bp, :, lanes(cp)])

    every = list(itertools.product(range(tx + 2), range(ty + 2)))
    own_places = [(ap, bp) for ap, bp in every if 1 <= ap <= tx and 1 <= bp <= ty]
    ghost_places = [p for p in every if p not in own_places]

    def split_ghosts(k):
        split_rows(k, own_places, (0, tz + 1))
        split_rows(k, ghost_places, range(tz + 2))

    charge_rows = lax.broadcasted_iota(jnp.int32, (4, tile), 0) < 2
    low_side = [m > 0 for m in me]
    high_side = [m < n - 1 for m, n in zip(me, counts)]

    def neighbours(a, b):
        groups = {}
        for ap, bp in itertools.product(range(a, a + 3), range(b, b + 3)):
            key = (
                -1 if ap == 0 else int(ap == tx + 1),
                -1 if bp == 0 else int(bp == ty + 1),
            )
            groups.setdefault(key, []).append((ap, bp))
        return groups

    tiles_of = [(a, b, (a * ty + b) * tz) for a, b in itertools.product(range(tx), range(ty))]

    def gather(k, a, b, base, pairs, c, first):
        left = jnp.concatenate(
            [lhs[k % 2, ap, bp, c + n] for ap, bp in pairs for n in range(3)], axis=1
        )
        right = jnp.concatenate(
            [
                store[base + c, pl.ds(((ap - a) * 3 + bp - b) * 3 * tile, 3 * tile), :]
                for ap, bp in pairs
            ],
            axis=0,
        )
        got = jnp.dot(left, right, preferred_element_type=f32)
        acc[base + c] = got if first else acc[base + c] + got

    def operate_inside(k):
        for a, b, base in tiles_of:
            for c in range(1, tz - 1):
                gather(k, a, b, base, neighbours(a, b)[0, 0], c, True)

    def operate_outside(k):
        norm = product = jnp.zeros((4, tile), f32)
        for a, b, base in tiles_of:
            groups = neighbours(a, b)
            for c in sorted({0, tz - 1}):
                gather(k, a, b, base, groups[0, 0], c, True)
            for key, pairs in groups.items():
                if key == (0, 0):
                    continue
                there = None
                for m, step in enumerate(key):
                    if step:
                        side = (low_side if step < 0 else high_side)[m]
                        there = side if there is None else there & side

                @pl.when(there)
                def _():
                    for c in range(tz):
                        gather(k, a, b, base, pairs, c, False)

            for c in range(tz):
                got = acc[base + c]
                pair = got[0:4] + got[4:8]
                pair = jnp.where(
                    charge_rows, pair[:, :tile] * coulomb_scale, pair[:, tile:] * -response_scale
                )
                here = lanes(c)
                if k == 0:
                    row_sums = jnp.where(
                        charge_rows,
                        got[8:12, :tile] * coulomb_scale + hard_ref[a, b, c : c + 1, :],
                        got[8:12, tile:] * response_scale + soft_ref[a, b, c : c + 1, :],
                    )
                    diag[a, b, :, here] = row_sums - SHIFT
                vector = basis[k, a + 1, b + 1, :, lanes(c + 1)]
                swapped = jnp.concatenate([vector[2:4], vector[0:2]], axis=0)
                link = coup_ref[a, b, c : c + 1, :]
                image = diag[a, b, :, here] * vector + pair + link * swapped
                if k + 1 < ITERS:
                    basis[k + 1, a + 1, b + 1, :, lanes(c + 1)] = image
                    lhs[(k + 1) % 2, a + 1, b + 1, c + 1] = split(image)
                else:
                    last[a, b, :, here] = image
                norm = norm + image * image
                product = product + vector * image
        return norm, product

    start_norm = jnp.zeros((4, tile), f32)
    for a, b, c in itertools.product(range(tx), range(ty), range(tz)):
        value = basis[0, a + 1, b + 1, :, lanes(c + 1)]
        start_norm = start_norm + value * value
    moments = {0: start_norm}
    split_rows(0, own_places, range(1, tz + 1))
    for k in range(ITERS):
        operate_inside(k)
        halo_wait(basis.at[k], 1 + k)
        split_ghosts(k)
        norm, product = operate_outside(k)
        moments[2 * k + 1] = product
        if k + 1 < ITERS:
            moments[2 * k + 2] = norm
            halo_start(basis.at[k + 1], 2 + k)
        if k + 2 == ITERS:
            sum_start(0, moments)
            early, moments = list(moments), {}
    sum_start(1, moments)
    gram = sum_finish(0, early)
    gram.update(sum_finish(1, list(moments)))
    gram = {n: jnp.broadcast_to(value, (4, tile)) for n, value in gram.items()}

    def dot(left, right):
        total = None
        for (i, x), (j, y) in itertools.product(enumerate(left), enumerate(right)):
            term = x * y * gram[i + j]
            total = term if total is None else total + term
        return total

    def combined(left, scale, right):
        size = max(len(left), len(right))
        out = []
        for i in range(size):
            if i >= len(left):
                out.append(scale * right[i])
            elif i >= len(right):
                out.append(left[i])
            else:
                out.append(left[i] + scale * right[i])
        return out

    one = jnp.ones((4, tile), f32)
    rem, along, found = [one], [one], []
    norm_now = gram[0]
    for k in range(ITERS):
        image = combined([SHIFT * x for x in along], one, [jnp.zeros_like(one)] + along)
        step_size = norm_now / dot(along, image)
        found = combined(found, step_size, along)
        rem = combined(rem, -step_size, image)
        if k + 1 < ITERS:
            norm_next = dot(rem, rem)
            along = combined(rem, norm_next / norm_now, along)
            norm_now = norm_next

    for a, b, c in itertools.product(range(tx), range(ty), range(tz)):
        held = [basis[k, a + 1, b + 1, :, lanes(c + 1)] for k in range(ITERS)]
        held.append(last[a, b, :, lanes(c)])
        out_ref[0, :, a, b, c, :] = sum(x * v for x, v in zip(found, held))
        out_ref[1, :, a, b, c, :] = sum(x * v for x, v in zip(rem, held))


def on_device(counts, positions, shield, width, hardness, softness, coupling, pair_bits, right_side):
    tx, ty, tz, tile = hardness.shape
    padded = (tx + 2, ty + 2)
    width_lanes = (tz + 2) * tile
    peers = counts[0] * counts[1] * counts[2]
    field = jax.ShapeDtypeStruct((2, 4, tx, ty, tz, tile), jnp.float32)
    vmem = pl.BlockSpec(memory_space=pltpu.VMEM)
    out = pl.pallas_call(
        functools.partial(kernel, counts, (tx, ty, tz), tile),
        out_shape=field,
        in_specs=[pl.BlockSpec(memory_space=pltpu.SMEM)] + [vmem] * 7,
        out_specs=vmem,
        scratch_shapes=[
            pltpu.VMEM((tx * ty * tz, 27 * tile, 2 * tile), jnp.bfloat16),
            pltpu.VMEM(padded + (8, width_lanes), jnp.float32),
            pltpu.VMEM((ITERS,) + padded + (4, width_lanes), jnp.float32),
            pltpu.VMEM((tx, ty, 4, tz * tile), jnp.float32),
            pltpu.VMEM((2,) + padded + (tz + 2, 16, tile), jnp.bfloat16),
            pltpu.VMEM((tz + 2, tile, 32), jnp.bfloat16),
            pltpu.VMEM((tz + 2, tile, 2 * tile), jnp.float32),
            pltpu.VMEM((32, 2 * tile), jnp.bfloat16),
            pltpu.VMEM((2 * 3 * tz, tile, tile), jnp.float32),
            pltpu.VMEM((tx * ty * tz, 16, 2 * tile), jnp.float32),
            pltpu.VMEM((tx, ty, 4, tz * tile), jnp.float32),
            pltpu.VMEM((2, 1, tile), jnp.float32),
            pltpu.VMEM((2, peers, 1, tile), jnp.float32),
            pltpu.SemaphoreType.DMA((ITERS + 1, 26)),
            pltpu.SemaphoreType.DMA((ITERS + 1, 26)),
            pltpu.SemaphoreType.DMA((2, peers)),
            pltpu.SemaphoreType.DMA((2, peers)),
        ],
        compiler_params=pltpu.CompilerParams(
            collective_id=0, has_side_effects=True, vmem_limit_bytes=67043328
        ),
    )(pair_bits, positions, shield, width, hardness, softness, coupling, right_side)
    return out[0], out[1]


def solution(mesh):
    counts = tuple(mesh.shape[axis] for axis in AXES)
    tiles = P("gx", "gy", "gz", None)
    four = P(None, "gx", "gy", "gz", None)
    return jax.shard_map(
        functools.partial(on_device, counts),
        mesh=mesh,
        in_specs=(four, tiles, tiles, tiles, tiles, tiles, P("gx", "gy", "gz"), four),
        out_specs=(four, four),
        check_vma=False,
    )
```

```python
import functools
import itertools
import math

import jax
import jax.numpy as jnp
from jax import lax
from jax.experimental import pallas as pl
from jax.experimental.pallas import tpu as pltpu
from jax.sharding import PartitionSpec as P

ITERS = 3
AXES = ("gx", "gy", "gz")
DIRECTIONS = [d for d in itertools.product((-1, 0, 1), repeat=3) if d != (0, 0, 0)]

LOG2E = math.log2(math.e)
coulomb_scale = 0.002 * math.sqrt(LOG2E)
response_scale = 0.003
SHIFT = 2.5


def sides(step, count, unit):
    if step < 0:
        return pl.ds(unit, unit), pl.ds((count + 1) * unit, unit)
    if step > 0:
        return pl.ds(count * unit, unit), pl.ds(0, unit)
    return pl.ds(unit, count * unit), pl.ds(unit, count * unit)


def kernel(
    counts, extent, tile,
    bits_ref, pos_ref, shield_ref, width_ref, hard_ref, soft_ref, coup_ref, rhs_ref,
    out_ref,
    store, par, basis, last, lhs, feats, columns, picker, energies, acc, diag, sums, parts,
    halo_send, halo_recv, sum_send, sum_recv,
):
    tx, ty, tz = extent
    bf16, f32 = jnp.bfloat16, jnp.float32
    me = [lax.axis_index(axis) for axis in AXES]
    inside = pl.ds(tile, tz * tile)

    def lanes(c, n=1):
        if isinstance(c, int):
            return pl.ds(c * tile, n * tile)
        return pl.ds(pl.multiple_of(c * tile, tile), n * tile)

    def exists(d):
        ok = None
        for m, step, count in zip(me, d, counts):
            if step:
                here = (m + step >= 0) & (m + step < count)
                ok = here if ok is None else ok & here
        return ok

    def halo_copy(ref, slot, index, d):
        pairs = [sides(s, n, u) for s, n, u in zip(d, extent, (1, 1, tile))]
        source = (pairs[0][0], pairs[1][0], slice(None), pairs[2][0])
        target = (pairs[0][1], pairs[1][1], slice(None), pairs[2][1])
        return pltpu.make_async_remote_copy(
            src_ref=ref.at[source],
            dst_ref=ref.at[target],
            send_sem=halo_send.at[slot, index],
            recv_sem=halo_recv.at[slot, index],
            device_id=tuple(m + s for m, s in zip(me, d)),
            device_id_type=pl.DeviceIdType.MESH,
        )

    def halo_start(ref, slot):
        for index, d in enumerate(DIRECTIONS):
            @pl.when(exists(d))
            def _():
                halo_copy(ref, slot, index, d).start()

    def halo_fill(ref, fill):
        for d in DIRECTIONS:
            back = tuple(-s for s in d)
            strips = [sides(s, n, u)[1] for s, n, u in zip(back, extent, (1, 1, tile))]

            @pl.when(jnp.logical_not(exists(d)))
            def _():
                region = (strips[0], strips[1], slice(None), strips[2])
                ref[region] = jnp.full(ref.at[region].shape, fill, f32)

    def halo_wait(ref, slot):
        for index, d in enumerate(DIRECTIONS):
            @pl.when(exists(d))
            def _():
                halo_copy(ref, slot, index, d).wait_send()

            back = tuple(-s for s in d)

            @pl.when(exists(back))
            def _():
                halo_copy(ref, slot, index, d).wait_recv()

    rank = (me[0] * counts[1] + me[1]) * counts[2] + me[2]
    hops = [h for h in itertools.product(*map(range, counts)) if any(h)]

    def sum_copies(slot):
        return [
            pltpu.make_async_remote_copy(
                src_ref=sums.at[slot],
                dst_ref=parts.at[slot, rank],
                send_sem=sum_send.at[slot, j],
                recv_sem=sum_recv.at[slot, j],
                device_id=tuple(lax.rem(m + h, n) for m, h, n in zip(me, hop, counts)),
                device_id_type=pl.DeviceIdType.MESH,
            )
            for j, hop in enumerate(hops)
        ]

    column = lax.broadcasted_iota(jnp.int32, (4, tile), 1)
    field = lax.broadcasted_iota(jnp.int32, (4, tile), 0)

    def sum_start(slot, values):
        packed = jnp.zeros((4, tile), f32)
        for place, value in values.items():
            total = jnp.sum(value, axis=1, keepdims=True)
            packed = jnp.where(column == 4 * place + field, total, packed)
        packed = jnp.sum(packed, axis=0, keepdims=True)
        sums[slot] = packed
        parts[slot, rank] = packed
        for copy in sum_copies(slot):
            copy.start()

    def sum_finish(slot, places):
        for copy in sum_copies(slot):
            copy.wait()
        value = jnp.broadcast_to(jnp.sum(parts[slot], axis=0), (4, tile))
        value = jnp.where(column % 2 == field % 2, value, 0.0)
        return {
            place: jnp.sum(jnp.where(column // 4 == place, value, 0.0), axis=1, keepdims=True)
            for place in places
        }

    barrier = pltpu.get_barrier_semaphore()
    for hop in hops:
        pl.semaphore_signal(
            barrier,
            inc=1,
            device_id=tuple(lax.rem(m + h, n) for m, h, n in zip(me, hop, counts)),
            device_id_type=pl.DeviceIdType.MESH,
        )

    row = lax.broadcasted_iota(jnp.int32, (8, tile), 0)
    blank = jnp.zeros((3, tile), f32)
    for a, b, c in itertools.product(range(tx), range(ty), range(tz)):
        par[a + 1, b + 1, :, lanes(c + 1)] = jnp.concatenate(
            [
                pos_ref[:, a, b, c, :] - 0.5,
                shield_ref[a, b, c : c + 1, :] * math.sqrt(LOG2E),
                width_ref[a, b, c : c + 1, :],
                blank,
            ],
            axis=0,
        )
        basis[0, a + 1, b + 1, :, lanes(c + 1)] = rhs_ref[:, a, b, c, :]
    halo_fill(par, 0.5)
    for k in range(ITERS):
        halo_fill(basis.at[k], 0.0)

    def rounded(value):
        return value.astype(bf16).astype(f32)

    slab = lax.broadcasted_iota(jnp.int32, (32, 2 * tile), 0)
    half = lax.broadcasted_iota(jnp.int32, (32, 2 * tile), 1) // tile
    picker[...] = jnp.where((slab >= 8) & (slab % 8 == 3 + half), 1.0, 0.0).astype(bf16)

    def prepare(ap, bp, cp):
        raw = par[ap, bp, :, lanes(cp)]
        scaled = raw * (2 * LOG2E)
        high = rounded(scaled)
        low = scaled - high
        squares = raw * raw
        norm = (squares[0:1] + squares[1:2] + squares[2:3]) * -LOG2E
        norm_high = rounded(norm)
        first = jnp.where(
            row < 3, high, jnp.where(row == 3, norm_high, jnp.where(row == 4, norm - norm_high, 1.0))
        )
        part = rounded(raw)
        rest = raw - part
        middle = rounded(rest)
        second = jnp.where(row < 3, high, jnp.where(row < 5, part, 0.0))
        third = jnp.where(row < 3, low, jnp.where(row < 5, middle, 0.0))
        fourth = jnp.where(row < 3, low, jnp.where(row < 5, rest - middle, 0.0))
        turned = jnp.concatenate([first, second, third, fourth], axis=0).T.astype(bf16)
        feats[cp] = turned
        columns[cp] = jnp.dot(turned, picker[...], preferred_element_type=f32)

    same = lax.broadcasted_iota(jnp.int32, (tile, tile), 0) == lax.broadcasted_iota(
        jnp.int32, (tile, tile), 1
    )

    def place_of(ap, bp, a, b):
        oa, ob = ap - 1 - a, bp - 1 - b
        group = (oa + 1) * 3 + (ob + 1)
        return oa, ob, group, (a * ty + b) * tz

    def cells_of(cp):
        return [c for c in (cp - 2, cp - 1, cp) if 0 <= c < tz]

    def measure_rows(ap, bp, a, b, sources, slot):
        oa, ob, group, _ = place_of(ap, bp, a, b)
        fa, fb = oa.astype(f32), ob.astype(f32)
        offset = jnp.where(row == 0, fa, jnp.where(row == 1, fb, 0.0))

        def target(c):
            own = par[a + 1, b + 1, :, lanes(c + 1)]
            grid = jnp.round(own * 128.0) * (1.0 / 128.0)
            rest = own - grid
            moved = own - offset
            squares = moved * moved
            plane = squares[0:1] + squares[1:2]
            bits = bits_ref[a, b, c]
            return own, grid - offset, jnp.where(row < 3, rest, 0.0), plane, own[2:3], bits

        def factors(parts_of, step):
            own, grid, rest, plane, height, bits = parts_of
            shifted = jnp.where(row == 2, grid - float(step), grid)
            norm = (plane + (height - float(step)) * (height - float(step))) * -LOG2E
            norm_high = rounded(norm)
            listed = (jnp.right_shift(bits, group * 3 + (step + 1)) & 1) == 1
            mask = jnp.where(listed, 0.0, -jnp.inf)
            first = jnp.where(row < 3, shifted, jnp.where(row < 5, 1.0, mask))
            first = jnp.where(row == 5, norm_high, jnp.where(row == 6, norm - norm_high, first))
            third = jnp.where(row < 3, shifted, 0.0)
            return jnp.concatenate([first, rest, third, rest], axis=0).astype(bf16)

        held = {}
        for cp in sources:
            cells = cells_of(cp)
            for c in cells:
                if c not in held:
                    held[c] = target(c)
            right = jnp.concatenate([factors(held[c], cp - 1 - c) for c in cells], axis=1)
            got = jnp.dot(feats[cp], right, preferred_element_type=f32)
            for m in range(len(cells)):
                energies[slot + m] = got[:, m * tile : (m + 1) * tile]
            slot += len(cells)

    def fill_rows(ap, bp, a, b, sources, slot):
        _, _, group, base = place_of(ap, bp, a, b)
        centre = group == 4
        for cp in sources:
            for c in cells_of(cp):
                own = par[a + 1, b + 1, :, lanes(c + 1)]
                energy = energies[slot].astype(bf16)
                slot += 1
                reach = (columns[cp, :, :tile] * own[3:4]).astype(bf16) - energy
                span = (columns[cp, :, tile:] + own[4:5]).astype(bf16)
                coulomb = lax.rsqrt(reach)
                response = jnp.exp2(energy / span)
                if cp - 1 == c:
                    drop = same & centre
                    coulomb = jnp.where(drop, jnp.zeros_like(coulomb), coulomb)
                    response = jnp.where(drop, jnp.zeros_like(response), response)
                start = group * (3 * tile) + (cp - c) * tile
                rows = pl.ds(pl.multiple_of(start, tile), tile)
                store[base + c, rows, :] = jnp.concatenate([coulomb, response], axis=1)

    def several(ap, bp, places, sources):
        each = sum(len(cells_of(cp)) for cp in sources)
        for n, (a, b) in enumerate(places):
            measure_rows(ap, bp, a, b, sources, n * each)
        for n, (a, b) in enumerate(places):
            fill_rows(ap, bp, a, b, sources, n * each)

    def source_row(ap, bp, sources, least=1):
        for cp in sources:
            prepare(ap, bp, cp)
        a_low, b_low = jnp.maximum(ap - 2, 0), jnp.maximum(bp - 2, 0)
        wide = jnp.minimum(bp, ty - 1) + 1 - b_low
        total = (jnp.minimum(ap, tx - 1) + 1 - a_low) * wide

        def place(n):
            return a_low + n // wide, b_low + n % wide

        def step(n, carry):
            several(ap, bp, [place(least * n + m) for m in range(least)], sources)
            return carry

        def single(n, carry):
            several(ap, bp, [place(total - 1)], sources)
            return carry

        lax.fori_loop(0, total // least, step, 0)
        if least == 2 and not (tx <= 2 and ty <= 2 and len(sources) == tz):
            lax.fori_loop(0, total % 2, single, 0)

    def own_rows(first, stop, sources, least):
        def over(q, carry):
            source_row(1 + q // ty, 1 + q % ty, sources, least)
            return carry

        lax.fori_loop(first, stop, over, 0)

    pairs = 2 if tx == 2 and ty == 2 else 1
    own_rows(0, 1, list(range(1, tz + 1)), pairs)
    pl.semaphore_wait(barrier, len(hops))
    halo_start(par, 0)
    halo_start(basis.at[0], 1)
    own_rows(1, tx * ty, list(range(1, tz + 1)), pairs)
    halo_wait(par, 0)
    own_rows(0, tx * ty, [0, tz + 1], 2 * pairs if pairs == 2 else 1)

    def ghost_row(q, carry):
        ap = q // (ty + 2)
        bp = q % (ty + 2)
        own = (ap >= 1) & (ap <= tx) & (bp >= 1) & (bp <= ty)
        held = (ap + me[0] >= 1) & (ap + me[0] <= tx + counts[0] - 1)
        held = held & (bp + me[1] >= 1) & (bp + me[1] <= ty + counts[1] - 1)

        @pl.when(jnp.logical_not(own) & held)
        def _():
            source_row(ap, bp, list(range(tz + 2)), 2)

        return carry

    lax.fori_loop(0, (tx + 2) * (ty + 2), ghost_row, 0)

    def split(value):
        upper = rounded(value)
        ones = jnp.ones((8, value.shape[1]), f32)
        return jnp.concatenate([upper, value - upper, ones], axis=0).astype(bf16)

    def split_rows(k, places, cells):
        for ap, bp in places:
            for cp in cells:
                lhs[k % 2, ap, bp, cp] = split(basis[k, ap, bp, :, lanes(cp)])

    every = list(itertools.product(range(tx + 2), range(ty + 2)))
    own_places = [(ap, bp) for ap, bp in every if 1 <= ap <= tx and 1 <= bp <= ty]
    ghost_places = [p for p in every if p not in own_places]

    def split_ghosts(k):
        split_rows(k, own_places, (0, tz + 1))
        split_rows(k, ghost_places, range(tz + 2))

    charge_rows = lax.broadcasted_iota(jnp.int32, (4, tile), 0) < 2
    low_side = [m > 0 for m in me]
    high_side = [m < n - 1 for m, n in zip(me, counts)]

    def neighbours(a, b):
        groups = {}
        for ap, bp in itertools.product(range(a, a + 3), range(b, b + 3)):
            key = (
                -1 if ap == 0 else int(ap == tx + 1),
                -1 if bp == 0 else int(bp == ty + 1),
            )
            groups.setdefault(key, []).append((ap, bp))
        return groups

    tiles_of = [(a, b, (a * ty + b) * tz) for a, b in itertools.product(range(tx), range(ty))]

    def gather(k, a, b, base, pairs, c, first):
        left = jnp.concatenate(
            [lhs[k % 2, ap, bp, c + n] for ap, bp in pairs for n in range(3)], axis=1
        )
        right = jnp.concatenate(
            [
                store[base + c, pl.ds(((ap - a) * 3 + bp - b) * 3 * tile, 3 * tile), :]
                for ap, bp in pairs
            ],
            axis=0,
        )
        got = jnp.dot(left, right, preferred_element_type=f32)
        acc[base + c] = got if first else acc[base + c] + got

    def operate_inside(k):
        for a, b, base in tiles_of:
            for c in range(1, tz - 1):
                gather(k, a, b, base, neighbours(a, b)[0, 0], c, True)

    def operate_outside(k):
        norm = product = jnp.zeros((4, tile), f32)
        for a, b, base in tiles_of:
            groups = neighbours(a, b)
            for c in sorted({0, tz - 1}):
                gather(k, a, b, base, groups[0, 0], c, True)
            for key, pairs in groups.items():
                if key == (0, 0):
                    continue
                there = None
                for m, step in enumerate(key):
                    if step:
                        side = (low_side if step < 0 else high_side)[m]
                        there = side if there is None else there & side

                @pl.when(there)
                def _():
                    for c in range(tz):
                        gather(k, a, b, base, pairs, c, False)

            for c in range(tz):
                got = acc[base + c]
                pair = got[0:4] + got[4:8]
                pair = jnp.where(
                    charge_rows, pair[:, :tile] * coulomb_scale, pair[:, tile:] * -response_scale
                )
                here = lanes(c)
                if k == 0:
                    row_sums = jnp.where(
                        charge_rows,
                        got[8:12, :tile] * coulomb_scale + hard_ref[a, b, c : c + 1, :],
                        got[8:12, tile:] * response_scale + soft_ref[a, b, c : c + 1, :],
                    )
                    diag[a, b, :, here] = row_sums - SHIFT
                vector = basis[k, a + 1, b + 1, :, lanes(c + 1)]
                swapped = jnp.concatenate([vector[2:4], vector[0:2]], axis=0)
                link = coup_ref[a, b, c : c + 1, :]
                image = diag[a, b, :, here] * vector + pair + link * swapped
                if k + 1 < ITERS:
                    basis[k + 1, a + 1, b + 1, :, lanes(c + 1)] = image
                    lhs[(k + 1) % 2, a + 1, b + 1, c + 1] = split(image)
                else:
                    last[a, b, :, here] = image
                norm = norm + image * image
                product = product + vector * image
        return norm, product

    start_norm = jnp.zeros((4, tile), f32)
    for a, b, c in itertools.product(range(tx), range(ty), range(tz)):
        value = basis[0, a + 1, b + 1, :, lanes(c + 1)]
        start_norm = start_norm + value * value
    moments = {0: start_norm}
    split_rows(0, own_places, range(1, tz + 1))
    for k in range(ITERS):
        operate_inside(k)
        halo_wait(basis.at[k], 1 + k)
        split_ghosts(k)
        norm, product = operate_outside(k)
        moments[2 * k + 1] = product
        if k + 1 < ITERS:
            moments[2 * k + 2] = norm
            halo_start(basis.at[k + 1], 2 + k)
    sum_start(0, moments)
    gram = sum_finish(0, list(moments))
    gram = {n: jnp.broadcast_to(value, (4, tile)) for n, value in gram.items()}

    def dot(left, right):
        total = None
        for (i, x), (j, y) in itertools.product(enumerate(left), enumerate(right)):
            term = x * y * gram[i + j]
            total = term if total is None else total + term
        return total

    def combined(left, scale, right):
        size = max(len(left), len(right))
        out = []
        for i in range(size):
            if i >= len(left):
                out.append(scale * right[i])
            elif i >= len(right):
                out.append(left[i])
            else:
                out.append(left[i] + scale * right[i])
        return out

    one = jnp.ones((4, tile), f32)
    rem, along, found = [one], [one], []
    norm_now = gram[0]
    for k in range(ITERS):
        image = combined([SHIFT * x for x in along], one, [jnp.zeros_like(one)] + along)
        step_size = norm_now / dot(along, image)
        found = combined(found, step_size, along)
        rem = combined(rem, -step_size, image)
        if k + 1 < ITERS:
            norm_next = dot(rem, rem)
            along = combined(rem, norm_next / norm_now, along)
            norm_now = norm_next

    for a, b, c in itertools.product(range(tx), range(ty), range(tz)):
        held = [basis[k, a + 1, b + 1, :, lanes(c + 1)] for k in range(ITERS)]
        held.append(last[a, b, :, lanes(c)])
        out_ref[0, :, a, b, c, :] = sum(x * v for x, v in zip(found, held))
        out_ref[1, :, a, b, c, :] = sum(x * v for x, v in zip(rem, held))


def on_device(counts, positions, shield, width, hardness, softness, coupling, pair_bits, right_side):
    tx, ty, tz, tile = hardness.shape
    padded = (tx + 2, ty + 2)
    width_lanes = (tz + 2) * tile
    peers = counts[0] * counts[1] * counts[2]
    field = jax.ShapeDtypeStruct((2, 4, tx, ty, tz, tile), jnp.float32)
    vmem = pl.BlockSpec(memory_space=pltpu.VMEM)
    out = pl.pallas_call(
        functools.partial(kernel, counts, (tx, ty, tz), tile),
        out_shape=field,
        in_specs=[pl.BlockSpec(memory_space=pltpu.SMEM)] + [vmem] * 7,
        out_specs=vmem,
        scratch_shapes=[
            pltpu.VMEM((tx * ty * tz, 27 * tile, 2 * tile), jnp.bfloat16),
            pltpu.VMEM(padded + (8, width_lanes), jnp.float32),
            pltpu.VMEM((ITERS,) + padded + (4, width_lanes), jnp.float32),
            pltpu.VMEM((tx, ty, 4, tz * tile), jnp.float32),
            pltpu.VMEM((2,) + padded + (tz + 2, 16, tile), jnp.bfloat16),
            pltpu.VMEM((tz + 2, tile, 32), jnp.bfloat16),
            pltpu.VMEM((tz + 2, tile, 2 * tile), jnp.float32),
            pltpu.VMEM((32, 2 * tile), jnp.bfloat16),
            pltpu.VMEM((2 * 3 * tz, tile, tile), jnp.float32),
            pltpu.VMEM((tx * ty * tz, 16, 2 * tile), jnp.float32),
            pltpu.VMEM((tx, ty, 4, tz * tile), jnp.float32),
            pltpu.VMEM((1, 1, tile), jnp.float32),
            pltpu.VMEM((1, peers, 1, tile), jnp.float32),
            pltpu.SemaphoreType.DMA((ITERS + 1, 26)),
            pltpu.SemaphoreType.DMA((ITERS + 1, 26)),
            pltpu.SemaphoreType.DMA((1, peers)),
            pltpu.SemaphoreType.DMA((1, peers)),
        ],
        compiler_params=pltpu.CompilerParams(
            collective_id=0, has_side_effects=True, vmem_limit_bytes=67043328
        ),
    )(pair_bits, positions, shield, width, hardness, softness, coupling, right_side)
    return out[0], out[1]


def solution(mesh):
    counts = tuple(mesh.shape[axis] for axis in AXES)
    tiles = P("gx", "gy", "gz", None)
    four = P(None, "gx", "gy", "gz", None)
    return jax.shard_map(
        functools.partial(on_device, counts),
        mesh=mesh,
        in_specs=(four, tiles, tiles, tiles, tiles, tiles, P("gx", "gy", "gz"), four),
        out_specs=(four, four),
        check_vma=False,
    )
```
